256 devices in a mesh: tp: 4 (over x), rep: 64 (over y, z, core).
Axes of the slice: x: 4, y: 4, z: 8, core: 2. Of those that a mesh axis runs over, the one named last changes fastest.
Arguments:
- queries: bfloat16 [1024, 4096], P('rep', 'tp'), may hold values from -6 to 6
- new_keys: bfloat16 [1024, 2048], P('rep', 'tp'), may hold values from -6 to 6
- new_values: bfloat16 [1024, 2048], P('rep', 'tp'), may hold values from -6 to 6
- stored_keys: bfloat16 [1024, 16, 128, 128], P('rep', 'tp'), may hold values from -6 to 6
- stored_values: bfloat16 [1024, 16, 128, 128], P('rep', 'tp'), may hold values from -6 to 6
- lengths: int32 [1024], P('rep'), may hold values from 1 to 128
- out_proj: bfloat16 [4096, 4608], P('tp', 'rep'), may hold values from -0.09375 to 0.09375
- residual: bfloat16 [1024, 4608], P(None, 'rep'), may hold values from -4.5 to 4.5
- norm_gain: float32 [4608], replicated, may hold values from 0.1 to 1.9
- embedding: bfloat16 [256000, 4608], P(('tp', 'rep')), may hold values from -1.25 to 1.25
- targets: int32 [1024], replicated, may hold values from 0 to 255999
- old_sums: float32 [1024], P('rep'), may hold values from -3 to 0
- rewards: float32 [1024], P('rep'), may hold values from -6 to 6
- group_ids: int32 [1024], P('rep'), may hold values from 0 to 127, as said below
Outputs:
- logprob_sum: float32 [1024], P('rep')
- advantage: float32 [1024], P('rep')
The draws below stay inside these ranges and needn't reach their ends.
Inputs may be any that keep to these rules, and one draw needn't show every extreme that they name: `group_ids`: each id names exactly 8 continuations.
All inputs are finite; a program needn't handle non-finite values.
Results may differ from the reference program's by a relative error of at most 0.001.
Values may be sent and summed in bfloat16 or wider, within the bound.
No kernel may reach another device: no remote copies, remote signals or barrier semaphores. Data moves between devices by JAX's collectives and lax.ppermute only.
A program may use at most 64 MiB of HBM per device.

```python
import math
import jax
import jax.numpy as jnp
from jax import lax

D = 4608
QUERY_HEADS = 32
KEY_VALUE_HEADS = 16
HEAD_SIZE = 128
VOCAB = 256000
GROUP = 8
CACHE_SLOTS = 128
SAMPLE_COUNT = 1024
QW = 4096
KW = 2048
N_TP = 4
N_REP = 64


def draw_residual(key, part):
    first, second, third = jax.random.split(jax.random.fold_in(key, 11), 3)
    columns = jnp.arange(D, dtype=jnp.float32)
    rough = jnp.exp(jax.random.uniform(second, (D,), jnp.float32, math.log(0.7), math.log(1.4)))
    rows = jnp.exp(jax.random.uniform(third, (SAMPLE_COUNT, 1), jnp.float32, math.log(0.5), math.log(2.0)))
    base = jnp.clip(jax.random.normal(first, (SAMPLE_COUNT, D), jnp.float32), -4.0, 4.0)
    ramp = 0.04 * 10.0 ** (columns / D)
    return (base * (ramp * rough)[None, :] * rows).astype(jnp.bfloat16)


def draw_embedding(key, part):
    first, second = jax.random.split(jax.random.fold_in(key, 23), 2)
    rows = jnp.arange(VOCAB, dtype=jnp.float32) / VOCAB
    rough = jnp.exp(jax.random.uniform(second, (VOCAB,), jnp.float32, math.log(0.88), math.log(1.14)))
    base = jnp.clip(jax.random.normal(first, (VOCAB, D), jnp.float32), -4.0, 4.0)
    spread = jnp.sqrt(14.0 + 2.2 * rows)
    return (base * (spread * rough)[:, None] / math.sqrt(D)).astype(jnp.bfloat16)


def draw_group_ids(key, part):
    order = jax.random.permutation(jax.random.fold_in(key, 37), SAMPLE_COUNT)
    return (order // GROUP).astype(jnp.int32)


def touch_ends(values, key, low, high):
    spot = [jax.random.randint(jax.random.fold_in(key, axis), (), 0, length) for axis, length in enumerate(values.shape)]
    longest = values.shape.index(max(values.shape))
    neighbour = spot[:longest] + [(spot[longest] + 1) % values.shape[longest]] + spot[longest + 1:]
    return values.at[tuple(spot)].set(low).at[tuple(neighbour)].set(high)


def block_scale(rng, shape, cuts, smallest, largest):
    level, own = 1.0, jax.random.fold_in(rng, 6)
    for position, parts in cuts:
        steps = jnp.exp(jax.random.uniform(jax.random.fold_in(own, position), (parts,), jnp.float32, smallest / len(cuts), largest / len(cuts)))
        level = level * jnp.repeat(steps, shape[position] // parts).reshape([-1 if axis == position else 1 for axis in range(len(shape))])
    return level


def gaussian(rng, extent, deviation, reach, cuts=(), kind=jnp.bfloat16):
    drawn = deviation * jax.random.normal(rng, extent, jnp.float32)
    if cuts:
        drawn = drawn * block_scale(rng, extent, cuts, -0.22, 0.18)
    return jnp.clip(drawn, -reach, reach).astype(kind)


def setup_inputs(seed: int = 0) -> dict:
    arg_keys = jax.random.split(jax.random.key(seed), 15)
    return {
        "queries": gaussian(arg_keys[0], (SAMPLE_COUNT, QW), 1.0, 6.0, ((0, 64), (1, 4))),
        "new_keys": gaussian(arg_keys[1], (SAMPLE_COUNT, KW), 1.0, 6.0, ((0, 64), (1, 4))),
        "new_values": gaussian(arg_keys[2], (SAMPLE_COUNT, KW), 1.0, 6.0, ((0, 64), (1, 4))),
        "stored_keys": gaussian(arg_keys[3], (SAMPLE_COUNT, KEY_VALUE_HEADS, CACHE_SLOTS, HEAD_SIZE), 1.0, 6.0, ((0, 64), (1, 4))),
        "stored_values": gaussian(arg_keys[4], (SAMPLE_COUNT, KEY_VALUE_HEADS, CACHE_SLOTS, HEAD_SIZE), 1.0, 6.0, ((0, 64), (1, 4))),
        "lengths": touch_ends(jax.random.randint(arg_keys[5], (SAMPLE_COUNT,), 1, CACHE_SLOTS + 1), jax.random.fold_in(arg_keys[5], 1), 1, CACHE_SLOTS).astype(jnp.int32),
        "out_proj": gaussian(arg_keys[6], (QW, D), QW ** -0.5, 0.09375, ((0, 4), (1, 64))),
        "residual": draw_residual(jax.random.fold_in(arg_keys[14], 71), 0),
        "norm_gain": jnp.clip(1.0 + 0.18 * jax.random.normal(arg_keys[8], (D,), jnp.float32), 0.1, 1.9),
        "embedding": draw_embedding(jax.random.fold_in(arg_keys[14], 71), 0),
        "targets": touch_ends(jax.random.randint(arg_keys[10], (SAMPLE_COUNT,), 0, VOCAB), jax.random.fold_in(arg_keys[10], 1), 0, VOCAB - 1).astype(jnp.int32),
        "old_sums": jnp.clip(-3.0 + 3.0 * jax.random.uniform(arg_keys[11], (SAMPLE_COUNT,), jnp.float32) ** block_scale(arg_keys[11], (SAMPLE_COUNT,), ((0, 64),), -0.2, 0.2), -3.0, 0.0),
        "rewards": gaussian(arg_keys[12], (SAMPLE_COUNT,), 1.0, 6.0, ((0, 64),), jnp.float32),
        "group_ids": draw_group_ids(jax.random.fold_in(arg_keys[14], 71), 0),
    }


def attend_one(items):
    query_vector, fresh_key, fresh_value, keys, values, length = items
    sample_ratio = QUERY_HEADS // KEY_VALUE_HEADS
    query_float = query_vector.astype(jnp.float32).reshape(KEY_VALUE_HEADS, sample_ratio, HEAD_SIZE)
    scores = jnp.einsum('gqd,gpd->gqp', query_float, keys.astype(jnp.float32)) / 12.0
    scores = 50.0 * jnp.tanh(scores / 50.0)
    valid = jnp.arange(CACHE_SLOTS, dtype=jnp.int32) < length
    expo = jnp.where(valid[None, None, :], jnp.exp(scores), 0.0)
    own_logit = jnp.einsum('xvi,xi->xv', query_float, fresh_key.astype(jnp.float32).reshape(KEY_VALUE_HEADS, HEAD_SIZE)) / 12.0
    own_logit = 50.0 * jnp.tanh(own_logit / 50.0)
    own_exp = jnp.exp(own_logit)
    total = lax.optimization_barrier(jnp.sum(expo, -1)) + own_exp
    probs = (expo / total[..., None]).astype(jnp.bfloat16)
    own_probability = (own_exp / total).astype(jnp.bfloat16)
    attended_output = jnp.einsum('gqp,gpd->gqd', probs.astype(jnp.float32), values.astype(jnp.float32))
    attended_output = attended_output + own_probability.astype(jnp.float32)[..., None] * fresh_value.astype(jnp.float32).reshape(KEY_VALUE_HEADS, 1, HEAD_SIZE)
    return attended_output.reshape(QUERY_HEADS * HEAD_SIZE).astype(jnp.bfloat16)

def reference(queries, new_keys, new_values, stored_keys, stored_values, lengths, out_proj, residual, norm_gain, embedding, targets, old_sums, rewards, group_ids):
    context = lax.map(attend_one, (queries, new_keys, new_values, stored_keys, stored_values, lengths))
    stream = residual.astype(jnp.float32) + jnp.dot(context, out_proj, preferred_element_type=jnp.float32)
    scale = lax.rsqrt(lax.optimization_barrier(jnp.mean(stream * stream, axis=1, keepdims=True)) + 1e-06)
    normed = (stream * scale * norm_gain[None, :]).astype(jnp.bfloat16)
    pieces = N_TP * N_REP
    width = VOCAB // pieces
    blocks = embedding.reshape(pieces, width, D)
    starts = jnp.arange(pieces, dtype=jnp.int32) * width

    def visit(carry, item):
        total, picked = carry
        block, start = item
        logits = lax.dot_general(normed, block, (((1,), (1,)), ((), ())), preferred_element_type=jnp.float32)
        logits = 30.0 * jnp.tanh(logits / 30.0)
        ids = start + jnp.arange(width, dtype=jnp.int32)
        total = total + lax.optimization_barrier(jnp.sum(jnp.exp(logits), 1))
        picked = picked + lax.optimization_barrier(jnp.sum(jnp.where(ids[None, :] == targets[:, None], logits, 0.0), 1))
        return ((total, picked), None)
    zeros = jnp.zeros((SAMPLE_COUNT,), jnp.float32)
    (total, picked), _ = lax.scan(visit, (zeros, zeros), (blocks, starts))
    logprob_sum = old_sums + (picked - jnp.log(total))
    groups = SAMPLE_COUNT // GROUP
    member = group_ids[:, None] == jnp.arange(groups, dtype=jnp.int32)[None, :]
    totals = lax.optimization_barrier(jnp.sum(jnp.where(member, rewards[:, None], 0.0), 0))
    mine = lax.optimization_barrier(jnp.sum(jnp.where(member, totals[None, :], 0.0), 1))
    advantage = rewards - (mine - rewards) / (GROUP - 1.0)
    return (logprob_sum, advantage)
```

```python
import functools

import jax
import jax.numpy as jnp
from jax import lax
from jax.experimental import pallas as pl
from jax.experimental.pallas import tpu as pltpu
from jax.sharding import Mesh
from jax.sharding import PartitionSpec as P

D = 4608
GROUP = 8
REP = ("y", "z", "c")
TP_REP = ("x", "y", "z", "c")
BF16 = jnp.bfloat16
F32 = jnp.float32


def shifted(x, axis, offset):
    n = lax.axis_size(axis)
    return lax.ppermute(x, axis, [((i + offset) % n, i) for i in range(n)])


def rolled(x, start, dim):
    n = x.shape[dim]
    return lax.dynamic_slice_in_dim(jnp.concatenate([x, x], dim), start, n, dim)


NT = (((1,), (1,)), ((), ()))
VMEM = pl.BlockSpec(memory_space=pltpu.VMEM)
SMEM = pl.BlockSpec(memory_space=pltpu.SMEM)


def attention_kernel(
    lengths_ref, q_ref, nk_ref, nv_ref, k_hbm, v_hbm, out_ref, k_ref, v_ref, k_sem, v_sem
):
    kv, samp, span, depth = k_ref.shape
    copies, ratio = out_ref.shape[0], q_ref.shape[1] // (kv * depth)
    k_copy = [pltpu.make_async_copy(k_hbm.at[:, g], k_ref.at[g], k_sem.at[g]) for g in range(kv)]
    v_copy = [pltpu.make_async_copy(v_hbm.at[:, g], v_ref.at[g], v_sem.at[g]) for g in range(kv)]
    for g in range(kv):
        k_copy[g].start()
        v_copy[g].start()
    row = lax.broadcasted_iota(jnp.int32, (ratio * samp, span), 0)
    slot = lax.broadcasted_iota(jnp.int32, (ratio * samp, span), 1)
    sample = lax.rem(row, samp)
    live = jnp.concatenate([lengths_ref[...]] * ratio, 0)
    for g in range(kv):
        heads = [pl.ds((g * ratio + r) * depth, depth) for r in range(ratio)]
        q = jnp.concatenate([q_ref[:, h].astype(F32) for h in heads], 0)
        q16 = q.astype(BF16)
        nk = jnp.concatenate([nk_ref[:, pl.ds(g * depth, depth)].astype(F32)] * ratio, 0)
        nv = jnp.concatenate([nv_ref[:, pl.ds(g * depth, depth)].astype(F32)] * ratio, 0)
        k_copy[g].wait()
        scores = jnp.zeros((ratio * samp, span), F32)
        for s in range(samp):
            found = lax.dot_general(q16, k_ref[g, s], NT, preferred_element_type=F32)
            scores = jnp.where(sample == s, found, scores)
        scores = 50.0 * jnp.tanh(scores / 12.0 / 50.0)
        expo = jnp.where(slot < live, jnp.exp(scores), 0.0)
        own = jnp.sum(q * nk, 1, keepdims=True)
        own = jnp.exp(50.0 * jnp.tanh(own / 12.0 / 50.0))
        total = jnp.sum(expo, 1, keepdims=True) + own
        probs = (expo / total).astype(BF16)
        own_prob = (own / total).astype(BF16).astype(F32)
        v_copy[g].wait()
        out = own_prob * nv
        found = jnp.zeros_like(out)
        for s in range(samp):
            one = jnp.dot(probs, v_ref[g, s], preferred_element_type=F32)
            found = jnp.where(sample == s, one, found)
        out = (found + out).astype(BF16)
        for r in range(ratio):
            for i in range(copies):
                out_ref[i, :, heads[r]] = out[r * samp : (r + 1) * samp]


def attention(queries, new_keys, new_values, stored_keys, stored_values, lengths, copies):
    samp, kv, span, depth = stored_keys.shape
    hbm = pl.BlockSpec(memory_space=pltpu.HBM)
    return pl.pallas_call(
        attention_kernel,
        out_shape=jax.ShapeDtypeStruct((copies, *queries.shape), BF16),
        in_specs=[VMEM, VMEM, VMEM, VMEM, hbm, hbm],
        out_specs=VMEM,
        scratch_shapes=[
            pltpu.VMEM((kv, samp, span, depth), BF16),
            pltpu.VMEM((kv, samp, span, depth), BF16),
            pltpu.SemaphoreType.DMA((kv,)),
            pltpu.SemaphoreType.DMA((kv,)),
        ],
        compiler_params=pltpu.CompilerParams(vmem_limit_bytes=58 << 20),
        cost_estimate=pl.CostEstimate(
            flops=4 << 30, bytes_accessed=4 << 20, transcendentals=1 << 16
        ),
        name="attend",
    )(lengths.reshape(samp, 1), queries, new_keys, new_values, stored_keys, stored_values)


def stream_kernel(at_ref, a_ref, b_ref, c_ref, d_ref, res_ref, gain_ref, out_ref, *, samp):
    rows, _ = a_ref.shape
    heads = (a_ref[...] + b_ref[...]) + (c_ref[...] + d_ref[...])
    res = jnp.concatenate([res_ref[i].astype(F32) for i in range(res_ref.shape[0])], 0).T
    half = res.shape[0] // 2
    res = jnp.where(at_ref[0] == 0, res[:half], res[half:])
    cores = half // rows
    units = []
    for u in range(rows // samp):
        at = u * cores * samp
        units.append(jnp.where(at_ref[1] == 0, res[at : at + samp], res[at + samp : at + 2 * samp]))
    value = ((heads + jnp.concatenate(units, 0)) * gain_ref[...]).astype(BF16)
    for i in range(out_ref.shape[0]):
        out_ref[i] = value


def assemble_kernel(got_ref, inverse_ref, out_ref, *, ny):
    nz, rows, wide = got_ref.shape
    width = wide // ny
    got = [got_ref[k].astype(F32) for k in range(nz)]
    pieces = [got[k][:, j * width : (j + 1) * width] for j in range(ny) for k in range(nz)]
    whole = jnp.concatenate(pieces, 1)
    out_ref[:, :D] = whole.astype(BF16)
    plain = whole * inverse_ref[...]
    scale = lax.rsqrt(jnp.sum(plain * plain, 1, keepdims=True) * (1.0 / D) + 1e-06) * (1.0 / 30.0)
    high = scale.astype(BF16).astype(F32)
    middle = (scale - high).astype(BF16).astype(F32)
    low = scale - high - middle
    lane = lax.broadcasted_iota(jnp.int32, (rows, out_ref.shape[1] - D), 1)
    tail = jnp.where(lane == 0, high, jnp.where(lane == 1, middle, jnp.where(lane == 2, low, 0.0)))
    out_ref[:, D:] = tail.astype(BF16)


def loss_kernel(*refs, blocks):
    base_ref, mark_ref, ready_ref, table_hbm = refs[:4]
    pieces = refs[4 : 4 + blocks]
    out_ref, rows_ref, table_ref, sem = refs[4 + blocks :]
    vocab = table_ref.shape[0]
    cuts = [*range(0, vocab, 512), vocab]
    parts = list(zip(cuts[:-1], cuts[1:]))
    copies = []
    for i, (lo, hi) in enumerate(parts):
        part = pl.ds(lo, hi - lo)
        copies.append(pltpu.make_async_copy(table_hbm.at[part], table_ref.at[part], sem.at[i]))
        copies[i].start()
    rows = 0
    for piece in pieces:
        rows_ref[rows : rows + piece.shape[0]] = piece[...]
        rows += piece.shape[0]
    scale = jnp.sum(rows_ref[:, D:].astype(F32), 1, keepdims=True)
    mark = mark_ref[...]
    total = jnp.zeros((rows, 1), F32)
    picked = jnp.zeros((rows, 1), F32)
    for which, ref in enumerate((ready_ref, table_ref)):
        for i, (lo, hi) in enumerate(parts):
            if which:
                copies[i].wait()
            acc = lax.dot_general(rows_ref[:, :D], ref[lo:hi], NT, preferred_element_type=F32)
            logits = 30.0 * jnp.tanh(acc * scale)
            ids = base_ref[1 - which] + lo + lax.broadcasted_iota(jnp.int32, (1, hi - lo), 1)
            total += jnp.sum(jnp.exp(logits), 1, keepdims=True)
            picked += jnp.sum(jnp.where(ids == mark, logits, 0.0), 1, keepdims=True)
    lane = lax.broadcasted_iota(jnp.int32, (rows, 128), 1)
    both = jnp.where(lane == 0, total, jnp.where(lane == 1, picked, 0.0))
    out_ref[...] = both.T[:8]


def losses(pieces, mark, tables, bases):
    rows = sum(p.shape[0] for p in pieces)
    vocab = tables[0].shape[0]
    return pl.pallas_call(
        functools.partial(loss_kernel, blocks=len(pieces)),
        out_shape=jax.ShapeDtypeStruct((8, rows), F32),
        in_specs=[SMEM, VMEM, VMEM, pl.BlockSpec(memory_space=pltpu.HBM)] + [VMEM] * len(pieces),
        out_specs=VMEM,
        scratch_shapes=[
            pltpu.VMEM((rows, pieces[0].shape[1]), BF16),
            pltpu.VMEM(tables[0].shape, BF16),
            pltpu.SemaphoreType.DMA((-(-vocab // 512),)),
        ],
        compiler_params=pltpu.CompilerParams(vmem_limit_bytes=36 << 20),
        cost_estimate=pl.CostEstimate(
            flops=4 * rows * vocab * D,
            bytes_accessed=4 * vocab * D,
            transcendentals=4 * rows * vocab,
        ),
    )(bases, mark.reshape(rows, 1), tables[1], tables[0], *pieces)


def per_device(
    queries,
    new_keys,
    new_values,
    stored_keys,
    stored_values,
    lengths,
    out_proj,
    residual,
    norm_gain,
    embedding,
    targets,
    old_sums,
    rewards,
    group_ids,
):
    nx, ny, nz, nc = (lax.axis_size(a) for a in TP_REP)
    x, y, z, c = (lax.axis_index(a) for a in TP_REP)
    samp = queries.shape[0]
    cols = out_proj.shape[1]
    vocab = embedding.shape[0]
    reps = ny * nz * nc
    groups = samp * reps // GROUP
    per_x = nz // nx
    rows = per_x * samp
    width = nc * cols

    other_embedding = shifted(embedding, "c", 1)
    proj, res = out_proj.T, residual.T
    feats, window = proj.shape[1], 2 * rows * nc

    def with_residual(k):
        start = ((y - k) % ny) * (nx * rows * nc) + (x // 2) * window
        return jnp.concatenate([proj, lax.dynamic_slice_in_dim(res, start, window, 1)], 1)

    both = [with_residual(0)] + [shifted(with_residual(k), "y", k) for k in range(1, ny)]
    both = rolled(jnp.stack(both), (ny - y) % ny, 0)
    both_other = shifted(both, "c", 1)
    both = jnp.where(
        c == 0, jnp.stack([both, both_other], 1), jnp.stack([both_other, both], 1)
    ).reshape(ny * nc, cols, feats + window)
    proj, res = both[:, :, :feats].reshape(ny * width, feats), both[:, :, feats:]
    context = attention(
        queries, new_keys, new_values, stored_keys, stored_values, lengths, nz
    )
    context = lax.all_to_all(context, "z", 0, 0, tiled=True).reshape(nz * samp, -1)

    member = group_ids[:, None] == lax.broadcasted_iota(jnp.int32, (1, groups), 1)
    reward_part = jnp.sum(jnp.where(member, rewards[:, None], 0.0), 0)
    reward_part = reward_part + shifted(reward_part, "c", 1)

    partial = lax.dot_general(context, proj, NT, preferred_element_type=F32)
    partial = partial.reshape(nx, rows, ny * width)

    def quarter(k):
        return lax.dynamic_index_in_dim(partial, (x + k) % nx, 0, False)

    heads = [quarter(0)] + [shifted(quarter(k), "x", -k) for k in range(1, nx)]
    gain = lax.dynamic_index_in_dim(norm_gain.reshape(ny, nz, width), z, 1, False)
    stream = pl.pallas_call(
        functools.partial(stream_kernel, samp=samp),
        out_shape=jax.ShapeDtypeStruct((nz, rows, ny * width), BF16),
        in_specs=[SMEM] + [VMEM] * 6,
        out_specs=VMEM,
        compiler_params=pltpu.CompilerParams(vmem_limit_bytes=8 << 20),
        name="stream",
    )(jnp.stack([x % 2, c]), *heads, res, gain.reshape(1, ny * width))
    stream = lax.all_to_all(stream, "z", 0, 0, tiled=True)

    block = pl.pallas_call(
        functools.partial(assemble_kernel, ny=ny),
        out_shape=jax.ShapeDtypeStruct((rows, D + 128), BF16),
        in_specs=[VMEM] * 2,
        out_specs=VMEM,
        compiler_params=pltpu.CompilerParams(vmem_limit_bytes=16 << 20),
        name="assemble",
    )(stream, (1.0 / norm_gain)[None])

    first, second = block[:samp], block[samp:]
    row_x, row_y = [first], [second]
    for k in range(1, nx):
        row_x.append(shifted(first, "x", k))
        row_y.append(shifted(second, "y", k))
    row_x, row_y = jnp.concatenate(row_x), jnp.concatenate(row_y)
    x_far, y_far = {0: row_x}, {0: row_y}
    for k in (1, nx - 1, 2):
        x_far[k], y_far[k] = shifted(row_x, "y", k), shifted(row_y, "x", k)

    marks = targets.reshape(ny, nx, per_x, nc, samp)
    marks = lax.dynamic_index_in_dim(marks, c, 3, False)
    marks = rolled(rolled(marks, y, 0), x, 1)
    marks_x = marks[:, :, 0].reshape(ny, nx * samp)
    marks_y = marks[:, :, 1].swapaxes(0, 1).reshape(nx, ny * samp)
    shard = (x * reps + (y * nz + z) * nc) * vocab
    bases = jnp.stack([shard + c * vocab, shard + (1 - c) * vocab])

    size = nx * samp
    part = {}
    for of in ((0,), (1, 3), (2,)):
        mark = jnp.concatenate([marks_x[k] for k in of] + [marks_y[k] for k in of])
        pieces = [x_far[k] for k in of] + [y_far[k] for k in of]
        found = losses(pieces, mark, (embedding, other_embedding), bases)
        for i, key in enumerate([("x", k) for k in of] + [("y", k) for k in of]):
            part[key] = found[:2, i * size : (i + 1) * size]
    half_x = jnp.stack([part["x", k] for k in range(ny)], 1).reshape(2, ny, nx, samp)
    half_y = jnp.stack([part["y", k] for k in range(nx)], 1).reshape(2, nx, ny, samp)
    half_y = half_y.swapaxes(1, 2)
    both = jnp.stack([half_x, half_y], 3)
    both = rolled(rolled(both, (ny - y) % ny, 1), (nx - x) % nx, 2)
    both = both.transpose(1, 2, 3, 0, 4).reshape(ny * nz, 2 * samp)
    both = jnp.broadcast_to(both[None], (nx, *both.shape)).reshape(nx * ny * nz, 2 * samp)
    spread = jnp.broadcast_to(reward_part[None], (nx * ny * nz, groups))
    payload = jnp.concatenate([both, spread], 1)
    payload = jnp.pad(payload, ((0, 0), (0, 256 - payload.shape[1])))[:, None]
    got = lax.all_to_all(payload, ("x", "y", "z"), 0, 0, tiled=True)[:, 0]
    sums = jnp.sum(got[:, : 2 * samp], 0)
    logprob_sum = old_sums + (sums[samp:] - jnp.log(sums[:samp]))
    group_total = jnp.sum(got[: ny * nz, 2 * samp : 2 * samp + groups], 0)
    mine = jnp.sum(jnp.where(member, group_total[None, :], 0.0), 1)
    advantage = rewards - (mine - rewards) / (GROUP - 1.0)
    return (logprob_sum, advantage)


def solution(mesh):
    split = Mesh(mesh.devices.reshape(mesh.shape["tp"], 4, 8, 2), TP_REP)
    placed = (
        P(REP, "x"),
        P(REP, "x"),
        P(REP, "x"),
        P(REP, "x", None, None),
        P(REP, "x", None, None),
        P(REP),
        P("x", REP),
        P(None, REP),
        P(),
        P(TP_REP, None),
        P(),
        P(REP),
        P(REP),
        P(REP),
    )

    return jax.shard_map(
        per_device, mesh=split, in_specs=placed, out_specs=(P(REP), P(REP)), check_vma=False
    )
```

```python
import functools

import jax
import jax.numpy as jnp
from jax import lax
from jax.experimental import pallas as pl
from jax.experimental.pallas import tpu as pltpu
from jax.sharding import Mesh
from jax.sharding import PartitionSpec as P

D = 4608
GROUP = 8
REP = ("y", "z", "c")
TP_REP = ("x", "y", "z", "c")
BF16 = jnp.bfloat16
F32 = jnp.float32


def shifted(x, axis, offset):
    n = lax.axis_size(axis)
    return lax.ppermute(x, axis, [((i + offset) % n, i) for i in range(n)])


def rolled(x, start, dim):
    n = x.shape[dim]
    return lax.dynamic_slice_in_dim(jnp.concatenate([x, x], dim), start, n, dim)


NT = (((1,), (1,)), ((), ()))
VMEM = pl.BlockSpec(memory_space=pltpu.VMEM)
SMEM = pl.BlockSpec(memory_space=pltpu.SMEM)


def attention_kernel(
    lengths_ref, q_ref, nk_ref, nv_ref, k_hbm, v_hbm, out_ref, k_ref, v_ref, k_sem, v_sem
):
    kv, samp, span, depth = k_ref.shape
    copies, ratio = out_ref.shape[0], q_ref.shape[1] // (kv * depth)
    k_copy = [pltpu.make_async_copy(k_hbm.at[:, g], k_ref.at[g], k_sem.at[g]) for g in range(kv)]
    v_copy = [pltpu.make_async_copy(v_hbm.at[:, g], v_ref.at[g], v_sem.at[g]) for g in range(kv)]
    for copy in k_copy + v_copy:
        copy.start()
    row = lax.broadcasted_iota(jnp.int32, (ratio * samp, span), 0)
    sample = lax.rem(row, samp)
    live = jnp.zeros((ratio * samp, span), jnp.int32)
    for s in range(samp):
        live = jnp.where(sample == s, lengths_ref[s], live)
    live = lax.broadcasted_iota(jnp.int32, live.shape, 1) < live
    heads = [[pl.ds((g * ratio + r) * depth, depth) for r in range(ratio)] for g in range(kv)]
    queries = [jnp.concatenate([q_ref[:, h].astype(F32) for h in heads[g]], 0) for g in range(kv)]

    def repeated(ref, g):
        return jnp.concatenate([ref[:, pl.ds(g * depth, depth)].astype(F32)] * ratio, 0)

    probs, own_probs = [], []
    for g in range(kv):
        own = jnp.sum(queries[g] * repeated(nk_ref, g), 1, keepdims=True)
        own_probs.append(jnp.exp(50.0 * jnp.tanh(own / 12.0 / 50.0)))
    for g in range(kv):
        k_copy[g].wait()
    for g in range(kv):
        q = queries[g].astype(BF16)
        scores = jnp.zeros(live.shape, F32)
        for s in range(samp):
            found = lax.dot_general(q, k_ref[g, s], NT, preferred_element_type=F32)
            scores = jnp.where(sample == s, found, scores)
        probs.append(scores)
    for g in range(kv):
        expo = jnp.where(live, jnp.exp(50.0 * jnp.tanh(probs[g] / 12.0 / 50.0)), 0.0)
        total = jnp.sum(expo, 1, keepdims=True) + own_probs[g]
        probs[g] = (expo / total).astype(BF16)
        own_probs[g] = (own_probs[g] / total).astype(BF16).astype(F32)
    for g in range(kv):
        v_copy[g].wait()
    for g in range(kv):
        found = jnp.zeros((ratio * samp, depth), F32)
        for s in range(samp):
            one = jnp.dot(probs[g], v_ref[g, s], preferred_element_type=F32)
            found = jnp.where(sample == s, one, found)
        out = (found + own_probs[g] * repeated(nv_ref, g)).astype(BF16)
        for r in range(ratio):
            for i in range(copies):
                out_ref[i, :, heads[g][r]] = out[r * samp : (r + 1) * samp]


def attention(queries, new_keys, new_values, stored_keys, stored_values, lengths, copies):
    samp, kv, span, depth = stored_keys.shape
    hbm = pl.BlockSpec(memory_space=pltpu.HBM)
    return pl.pallas_call(
        attention_kernel,
        out_shape=jax.ShapeDtypeStruct((copies, *queries.shape), BF16),
        in_specs=[SMEM, VMEM, VMEM, VMEM, hbm, hbm],
        out_specs=VMEM,
        scratch_shapes=[
            pltpu.VMEM((kv, samp, span, depth), BF16),
            pltpu.VMEM((kv, samp, span, depth), BF16),
            pltpu.SemaphoreType.DMA((kv,)),
            pltpu.SemaphoreType.DMA((kv,)),
        ],
        compiler_params=pltpu.CompilerParams(vmem_limit_bytes=58 << 20),
        cost_estimate=pl.CostEstimate(
            flops=4 << 30, bytes_accessed=4 << 20, transcendentals=1 << 16
        ),
        name="attend",
    )(lengths, queries, new_keys, new_values, stored_keys, stored_values)


def stream_kernel(at_ref, a_ref, b_ref, c_ref, d_ref, res_ref, gain_ref, out_ref, *, samp):
    rows, _ = a_ref.shape
    heads = (a_ref[...] + b_ref[...]) + (c_ref[...] + d_ref[...])
    res = jnp.concatenate([res_ref[i].astype(F32) for i in range(res_ref.shape[0])], 0).T
    half = res.shape[0] // 2
    res = jnp.where(at_ref[0] == 0, res[:half], res[half:])
    cores = half // rows
    units = []
    for u in range(rows // samp):
        at = u * cores * samp
        units.append(jnp.where(at_ref[1] == 0, res[at : at + samp], res[at + samp : at + 2 * samp]))
    value = ((heads + jnp.concatenate(units, 0)) * gain_ref[...]).astype(BF16)
    for i in range(out_ref.shape[0]):
        out_ref[i] = value


def assemble_kernel(got_ref, inverse_ref, out_ref, *, ny):
    nz, rows, wide = got_ref.shape
    width = wide // ny
    got = [got_ref[k].astype(F32) for k in range(nz)]
    pieces = [got[k][:, j * width : (j + 1) * width] for j in range(ny) for k in range(nz)]
    whole = jnp.concatenate(pieces, 1)
    out_ref[:, :D] = whole.astype(BF16)
    plain = whole * inverse_ref[...]
    scale = lax.rsqrt(jnp.sum(plain * plain, 1, keepdims=True) * (1.0 / D) + 1e-06) * (1.0 / 30.0)
    high = scale.astype(BF16).astype(F32)
    middle = (scale - high).astype(BF16).astype(F32)
    low = scale - high - middle
    lane = lax.broadcasted_iota(jnp.int32, (rows, out_ref.shape[1] - D), 1)
    tail = jnp.where(lane == 0, high, jnp.where(lane == 1, middle, jnp.where(lane == 2, low, 0.0)))
    out_ref[:, D:] = tail.astype(BF16)


def windows(vocab, size):
    starts = [min(at, vocab - size) for at in range(0, vocab, size)]
    return [(lo, at - lo) for lo, at in zip(starts, range(0, vocab, size))]


def loss_kernel(*refs, blocks, wide):
    base_ref, mark_ref, ready_ref, table_hbm = refs[:4]
    pieces = refs[4 : 4 + blocks]
    out_ref, rows_ref, table_ref, sem = refs[4 + blocks :]
    vocab = table_ref.shape[0]
    parts = windows(vocab, wide)
    copies = []
    for i, (lo, seen) in enumerate(parts):
        part = pl.ds(lo + seen, wide - seen)
        copies.append(pltpu.make_async_copy(table_hbm.at[part], table_ref.at[part], sem.at[i]))
        copies[i].start()
    rows = 0
    for piece in pieces:
        rows_ref[rows : rows + piece.shape[0]] = piece[...]
        rows += piece.shape[0]
    scale = jnp.sum(rows_ref[:, D:].astype(F32), 1, keepdims=True)
    lane = lax.broadcasted_iota(jnp.int32, (1, 128), 1)
    mark = mark_ref[...] - lane
    total = jnp.zeros((rows, 128), F32)
    picked = jnp.zeros((rows, 128), F32)
    for which, ref in enumerate((ready_ref, table_ref)):
        for i, (lo, seen) in enumerate(parts):
            if which:
                copies[i].wait()
            acc = lax.dot_general(
                rows_ref[:, :D], ref[lo : lo + wide], NT, preferred_element_type=F32
            )
            for at in range(0, wide, 128):
                if seen >= at + 128:
                    continue
                soft = jnp.tanh(acc[:, at : at + 128] * scale)
                expo = jnp.exp(30.0 * soft)
                found = jnp.where(mark == base_ref[1 - which] + (lo + at), soft, 0.0)
                if seen > at:
                    fresh = lane >= seen - at
                    expo = jnp.where(fresh, expo, 0.0)
                    found = jnp.where(fresh, found, 0.0)
                total += expo
                picked += found
    total = jnp.sum(total, 1, keepdims=True)
    picked = jnp.sum(picked, 1, keepdims=True) * 30.0
    both = jnp.where(lane == 0, total, jnp.where(lane == 1, picked, 0.0))
    out_ref[...] = both.T[:8]


def losses(pieces, mark, tables, bases):
    rows = sum(p.shape[0] for p in pieces)
    vocab = tables[0].shape[0]
    return pl.pallas_call(
        functools.partial(loss_kernel, blocks=len(pieces), wide=512),
        out_shape=jax.ShapeDtypeStruct((8, rows), F32),
        in_specs=[SMEM, VMEM, VMEM, pl.BlockSpec(memory_space=pltpu.HBM)] + [VMEM] * len(pieces),
        out_specs=VMEM,
        scratch_shapes=[
            pltpu.VMEM((rows, pieces[0].shape[1]), BF16),
            pltpu.VMEM(tables[0].shape, BF16),
            pltpu.SemaphoreType.DMA((-(-vocab // 512),)),
        ],
        compiler_params=pltpu.CompilerParams(vmem_limit_bytes=36 << 20),
        cost_estimate=pl.CostEstimate(
            flops=4 * rows * vocab * D,
            bytes_accessed=4 * vocab * D,
            transcendentals=4 * rows * vocab,
        ),
    )(bases, mark.reshape(rows, 1), tables[1], tables[0], *pieces)


def per_device(
    queries,
    new_keys,
    new_values,
    stored_keys,
    stored_values,
    lengths,
    out_proj,
    residual,
    norm_gain,
    embedding,
    targets,
    old_sums,
    rewards,
    group_ids,
):
    nx, ny, nz, nc = (lax.axis_size(a) for a in TP_REP)
    x, y, z, c = (lax.axis_index(a) for a in TP_REP)
    samp = queries.shape[0]
    cols = out_proj.shape[1]
    vocab = embedding.shape[0]
    reps = ny * nz * nc
    groups = samp * reps // GROUP
    per_x = nz // nx
    rows = per_x * samp
    width = nc * cols

    other_embedding = shifted(embedding, "c", 1)
    context = attention(
        queries, new_keys, new_values, stored_keys, stored_values, lengths, nz
    )
    out_proj, residual, context = lax.optimization_barrier((out_proj, residual, context))
    proj, res = out_proj.T, residual.T
    feats, window = proj.shape[1], 2 * rows * nc

    def with_residual(k):
        start = ((y - k) % ny) * (nx * rows * nc) + (x // 2) * window
        return jnp.concatenate([proj, lax.dynamic_slice_in_dim(res, start, window, 1)], 1)

    both = [with_residual(0)] + [shifted(with_residual(k), "y", k) for k in range(1, ny)]
    both = rolled(jnp.stack(both), (ny - y) % ny, 0)
    both_other = shifted(both, "c", 1)
    both = jnp.where(
        c == 0, jnp.stack([both, both_other], 1), jnp.stack([both_other, both], 1)
    ).reshape(ny * nc, cols, feats + window)
    proj, res = both[:, :, :feats].reshape(ny * width, feats), both[:, :, feats:]

    context = lax.all_to_all(context, "z", 0, 0, tiled=True).reshape(nz * samp, -1)

    member = group_ids[:, None] == lax.broadcasted_iota(jnp.int32, (1, groups), 1)
    reward_part = jnp.sum(jnp.where(member, rewards[:, None], 0.0), 0)
    reward_part = reward_part + shifted(reward_part, "c", 1)

    partial = lax.dot_general(context, proj, NT, preferred_element_type=F32)
    partial = partial.reshape(nx, rows, ny * width)

    def quarter(k):
        return lax.dynamic_index_in_dim(partial, (x + k) % nx, 0, False)

    heads = [quarter(0)] + [shifted(quarter(k), "x", -k) for k in range(1, nx)]
    gain = lax.dynamic_index_in_dim(norm_gain.reshape(ny, nz, width), z, 1, False)
    stream = pl.pallas_call(
        functools.partial(stream_kernel, samp=samp),
        out_shape=jax.ShapeDtypeStruct((nz, rows, ny * width), BF16),
        in_specs=[SMEM] + [VMEM] * 6,
        out_specs=VMEM,
        compiler_params=pltpu.CompilerParams(vmem_limit_bytes=8 << 20),
        name="stream",
    )(jnp.stack([x % 2, c]), *heads, res, gain.reshape(1, ny * width))
    stream = lax.all_to_all(stream, "z", 0, 0, tiled=True)

    block = pl.pallas_call(
        functools.partial(assemble_kernel, ny=ny),
        out_shape=jax.ShapeDtypeStruct((rows, D + 128), BF16),
        in_specs=[VMEM] * 2,
        out_specs=VMEM,
        compiler_params=pltpu.CompilerParams(vmem_limit_bytes=16 << 20),
        name="assemble",
    )(stream, (1.0 / norm_gain)[None])

    first, second = block[:samp], block[samp:]
    row_x, row_y = [first], [second]
    for k in range(1, nx):
        row_x.append(shifted(first, "x", k))
        row_y.append(shifted(second, "y", k))
    row_x, row_y = jnp.concatenate(row_x), jnp.concatenate(row_y)
    x_far, y_far = {0: row_x}, {0: row_y}
    for k in (1, nx - 1, 2):
        x_far[k], y_far[k] = shifted(row_x, "y", k), shifted(row_y, "x", k)

    marks = targets.reshape(ny, nx, per_x, nc, samp)
    marks = lax.dynamic_index_in_dim(marks, c, 3, False)
    marks = rolled(rolled(marks, y, 0), x, 1)
    marks_x = marks[:, :, 0].reshape(ny, nx * samp)
    marks_y = marks[:, :, 1].swapaxes(0, 1).reshape(nx, ny * samp)
    shard = (x * reps + (y * nz + z) * nc) * vocab
    bases = jnp.stack([shard + c * vocab, shard + (1 - c) * vocab])

    size = nx * samp
    part = {}
    for of in ((0,), (1, nx - 1, 2)):
        mark = jnp.concatenate([marks_x[k] for k in of] + [marks_y[k] for k in of])
        pieces = [x_far[k] for k in of] + [y_far[k] for k in of]
        found = losses(pieces, mark, (embedding, other_embedding), bases)
        for i, key in enumerate([("x", k) for k in of] + [("y", k) for k in of]):
            part[key] = found[:2, i * size : (i + 1) * size]
    half_x = jnp.stack([part["x", k] for k in range(ny)], 1).reshape(2, ny, nx, samp)
    half_y = jnp.stack([part["y", k] for k in range(nx)], 1).reshape(2, nx, ny, samp)
    half_y = half_y.swapaxes(1, 2)
    both = jnp.stack([half_x, half_y], 3)
    both = rolled(rolled(both, (ny - y) % ny, 1), (nx - x) % nx, 2)
    both = both.transpose(1, 2, 3, 0, 4).reshape(ny * nz, 2 * samp)
    both = jnp.broadcast_to(both[None], (nx, *both.shape)).reshape(nx * ny * nz, 2 * samp)
    spread = jnp.broadcast_to(reward_part[None], (nx * ny * nz, groups))
    payload = jnp.concatenate([both, spread], 1)
    payload = jnp.pad(payload, ((0, 0), (0, 256 - payload.shape[1])))[:, None]
    got = lax.all_to_all(payload, ("x", "y", "z"), 0, 0, tiled=True)[:, 0]
    sums = jnp.sum(got[:, : 2 * samp], 0)
    logprob_sum = old_sums + (sums[samp:] - jnp.log(sums[:samp]))
    group_total = jnp.sum(got[: ny * nz, 2 * samp : 2 * samp + groups], 0)
    mine = jnp.sum(jnp.where(member, group_total[None, :], 0.0), 1)
    advantage = rewards - (mine - rewards) / (GROUP - 1.0)
    return (logprob_sum, advantage)


def solution(mesh):
    split = Mesh(mesh.devices.reshape(mesh.shape["tp"], 4, 8, 2), TP_REP)
    placed = (
        P(REP, "x"),
        P(REP, "x"),
        P(REP, "x"),
        P(REP, "x", None, None),
        P(REP, "x", None, None),
        P(REP),
        P("x", REP),
        P(None, REP),
        P(),
        P(TP_REP, None),
        P(),
        P(REP),
        P(REP),
        P(REP),
    )

    return jax.shard_map(
        per_device, mesh=split, in_specs=placed, out_specs=(P(REP), P(REP)), check_vma=False
    )
```
